32 devices in a mesh: row: 8 (over z, y), col: 4 (over x, core).
Axes of the slice: x: 2, y: 2, z: 4, core: 2. Of those that a mesh axis runs over, the one named last changes fastest.
Arguments:
- spectrum: float32 [2, 4096, 2048], P(None, 'row', 'col'), may hold values from -6 to 6
- pupil: float32 [2, 512, 512], replicated, may hold values from -4.2 to 4.2
- amplitudes: float32 [8, 4, 1, 512, 512], P('row', 'col'), may hold values from 0.1 to 3
- offsets: int32 [8, 4, 1, 2], P('row', 'col'), may hold values from 0 to 511, as said below
- counts: int32 [8, 4], P('row', 'col'), may hold values from 1 to 1, as said below
Outputs:
- recovered: float32 [2, 4096, 2048], P(None, 'row', 'col')
The draws below stay inside these ranges and needn't reach their ends.
Inputs may be any that keep to these rules, and one draw needn't show every extreme that they name: `offsets`: offsets are corners inside the tile: the row below 512, the column below 512. `counts`: some device has all 1 slots live.
All inputs are finite; a program needn't handle non-finite values.
Results may differ from the reference program's by a relative error of at most 0.012.
Values sent between devices are 32-bit elements; how exact they have to be, the bound alone decides.
A program may use at most 128 MiB of HBM per device.

```python
import math
import jax
import jax.numpy as jnp
from jax import lax

W = 512
TR = 512
TC = 512
CAP = 1
SWEEPS = 2
NR = 4096
NC = 2048
N_ROW = 8
N_COL = 4


def draw_offsets(key, part):
    first = jax.random.randint(jax.random.fold_in(key, 11), (N_ROW, N_COL, CAP, 1), 0, TR)
    second = jax.random.randint(jax.random.fold_in(key, 12), (N_ROW, N_COL, CAP, 1), 0, TC)
    return jnp.concatenate([first, second], axis=3).astype(jnp.int32)


def draw_counts(key, part):
    base = jax.random.randint(jax.random.fold_in(key, 21), (N_ROW * N_COL,), 1, CAP + 1)
    chosen = jax.random.randint(jax.random.fold_in(key, 22), (), 0, N_ROW * N_COL)
    base = base.at[chosen].set(CAP)
    return base.reshape(N_ROW, N_COL).astype(jnp.int32)


def levels(own_key, dims, pieces, least, top_value):
    factor_of, own = 1.0, jax.random.fold_in(own_key, 6)
    for axis_at, blocks in pieces:
        draws = jnp.exp(jax.random.uniform(jax.random.fold_in(own, axis_at), (blocks,), jnp.float32, least / len(pieces), top_value / len(pieces)))
        factor_of = factor_of * jnp.repeat(draws, dims[axis_at] // blocks).reshape([-1 if axis == axis_at else 1 for axis in range(len(dims))])
    return factor_of


def normal_values(own_key, extent, scale, limit, shards=(), kind=jnp.bfloat16):
    drawn = scale * jax.random.normal(own_key, extent, jnp.float32)
    if shards:
        drawn = drawn * levels(own_key, extent, shards, -0.22, 0.18)
    return jnp.clip(drawn, -limit, limit).astype(kind)


def setup_inputs(seed: int = 0) -> dict:
    key_list = jax.random.split(jax.random.key(seed), 6)
    spectrum = normal_values(key_list[0], (2, NR, NC), 1.0, 6.0, ((1, 8), (2, 4)), jnp.float32)
    pupil = normal_values(key_list[1], (2, W, W), 0.7, 4.2, (), jnp.float32)
    amplitudes = jnp.clip(jnp.exp(math.log(3.0) - 3.4011974 * jax.random.uniform(key_list[2], (N_ROW, N_COL, CAP, W, W), jnp.float32) ** levels(key_list[2], (N_ROW, N_COL, CAP, W, W), ((0, 8), (1, 4)), -0.2, 0.2)), 0.1, 3.0)
    offsets = draw_offsets(jax.random.fold_in(key_list[5], 71), 0)
    counts = draw_counts(jax.random.fold_in(key_list[5], 71), 0)
    return {"spectrum": spectrum, "pupil": pupil, "amplitudes": amplitudes, "offsets": offsets, "counts": counts}


step_size = 0.5
floor_value = 0.05

def dft_tables(width):
    index = jnp.arange(width, dtype=jnp.int32)
    phase = index[:, None] * index[None, :] % width
    angle = phase.astype(jnp.float32) * (2.0 * math.pi / width)
    scale = 1.0 / math.sqrt(width)
    return ((jnp.cos(angle) * scale).astype(jnp.bfloat16), (jnp.sin(angle) * scale).astype(jnp.bfloat16))

def transform(real, imag, cosine, sine, sign):
    cosine = cosine.astype(jnp.float32)
    sine = sine.astype(jnp.float32)
    real = real.astype(jnp.bfloat16).astype(jnp.float32)
    imag = imag.astype(jnp.bfloat16).astype(jnp.float32)

    def right(a, b):
        return jnp.einsum('swk,kj->swj', a, b, precision=lax.Precision.HIGHEST)

    def left(b, a):
        return jnp.einsum('ik,skj->sij', b, a, precision=lax.Precision.HIGHEST)
    first_real = (right(real, cosine) - sign * right(imag, sine)).astype(jnp.bfloat16).astype(jnp.float32)
    first_imag = (right(imag, cosine) + sign * right(real, sine)).astype(jnp.bfloat16).astype(jnp.float32)
    out_real = left(cosine, first_real) - sign * left(sine, first_imag)
    out_imag = left(cosine, first_imag) + sign * left(sine, first_real)
    return (out_real, out_imag)

def slot_gradient(window_real, window_imag, pupil, amps, live, cosine, sine):
    pupil_real = pupil[0][None]
    pupil_imag = pupil[1][None]
    field_real = window_real * pupil_real - window_imag * pupil_imag
    field_imag = window_real * pupil_imag + window_imag * pupil_real
    wave_real, wave_imag = transform(field_real, field_imag, cosine, sine, 1.0)
    magnitude = jnp.sqrt(wave_real * wave_real + wave_imag * wave_imag)
    keep = 1.0 - amps / jnp.maximum(magnitude, floor_value)
    back_real, back_imag = transform(wave_real * keep, wave_imag * keep, cosine, sine, -1.0)
    mask = live[:, None, None]
    grad_real = (back_real * pupil_real + back_imag * pupil_imag) * mask
    grad_imag = (back_imag * pupil_real - back_real * pupil_imag) * mask
    return (grad_real, grad_imag)

def reference(spectrum, pupil, amplitudes, offsets, counts):
    cosine, sine = dft_tables(W)
    total_slots = N_ROW * N_COL * CAP
    flat_amps = amplitudes.reshape(total_slots, W, W)
    flat_offsets = offsets.reshape(total_slots, 2)
    flat_counts = counts.reshape(N_ROW * N_COL)
    for sweep in range(SWEEPS):
        padded = jnp.pad(spectrum, ((0, 0), (0, W), (0, W)))

        def one(index, total):
            device = index // CAP
            slot = index % CAP
            row_start = (device // N_COL * TR + flat_offsets[index, 0]).astype(jnp.int32)
            col_start = (device % N_COL * TC + flat_offsets[index, 1]).astype(jnp.int32)
            zero = jnp.zeros((), jnp.int32)
            window = lax.dynamic_slice(padded, (zero, row_start, col_start), (2, W, W))
            amp = lax.dynamic_slice_in_dim(flat_amps, index.astype(jnp.int32), 1, 0)
            live = (slot < flat_counts[device]).astype(jnp.float32)
            grad_real, grad_imag = slot_gradient(window[0][None], window[1][None], pupil, amp, live[None], cosine, sine)
            piece = jnp.stack([grad_real[0], grad_imag[0]])
            current = lax.dynamic_slice(total, (zero, row_start, col_start), (2, W, W))
            return lax.dynamic_update_slice(total, current + piece, (zero, row_start, col_start))
        total = lax.fori_loop(jnp.int32(0), jnp.int32(total_slots), one, jnp.zeros_like(padded))
        spectrum = spectrum - step_size * total[:, :NR, :NC]
    return spectrum
```

```python
import functools
import math

import jax
import jax.numpy as jnp
import numpy as np
from jax import lax
from jax.experimental import pallas as pl
from jax.experimental.pallas import tpu as pltpu
from jax.sharding import PartitionSpec as P

SWEEPS = 2
CHUNKS = 8

step_size = 0.5
floor_value = 0.05

MESH = pl.DeviceIdType.MESH
BF16 = jnp.bfloat16
F32 = jnp.float32


def dft_tables(width):
    index = np.arange(width)
    angle = (index[:, None] * index[None, :] % width) * (2.0 * math.pi / width)
    scale = 1.0 / math.sqrt(width)
    return (
        jnp.asarray((np.cos(angle) * scale).astype(np.float32).astype(BF16)),
        jnp.asarray((np.sin(angle) * scale).astype(np.float32).astype(BF16)),
    )


def dot(a, b):
    return jnp.dot(a, b, preferred_element_type=F32)


def iota(shape, axis):
    return lax.broadcasted_iota(jnp.int32, shape, axis)


def kernel(
    n_row, n_col, offs, meta, spec, pupil, amps, cosine, sine, out,
    below1, right1, diag1, give1, got1, own, down1, above1, tile2,
    below2, right2, diag2, give2, got2, down2, above2,
    pup, fwd_right, fwd_left, back_right, back_left, f1, f2, hot, left_dr, send, recv, meta_sem,
):
    width = spec.shape[1]
    size = width // CHUNKS
    r, c = lax.axis_index("row"), lax.axis_index("col")
    has_up, has_down = r > 0, r < n_row - 1
    has_left, has_right = c > 0, c < n_col - 1
    up = (lax.rem(r + n_row - 1, n_row), c)
    down = (lax.rem(r + 1, n_row), c)
    left = (r, lax.rem(c + n_col - 1, n_col))
    right = (r, lax.rem(c + 1, n_col))
    dr, dc = offs[0], offs[1]
    live = offs[2].astype(F32)

    def ds(k, block=size, base=0):
        return pl.ds(pl.multiple_of(base + k * block, 8), block)

    def flow(kind, src, dst, device):
        def copy(k):
            return pltpu.make_async_remote_copy(
                src_ref=src.at[:, ds(k), :], dst_ref=dst.at[:, ds(k), :],
                send_sem=send.at[kind, k], recv_sem=recv.at[kind, k],
                device_id=device, device_id_type=MESH,
            )
        return copy

    def each(body, count=CHUNKS):
        def step(k, carry):
            body(k)
            return carry
        lax.fori_loop(0, count, step, 0)

    neighbours = ((has_up, up), (has_down, down), (has_left, left), (has_right, right))
    barrier = pltpu.get_barrier_semaphore()
    for there, device in neighbours:
        @pl.when(there)
        def _():
            pl.semaphore_signal(barrier, inc=1, device_id=device, device_id_type=MESH)
    pl.semaphore_wait(barrier, sum(there.astype(jnp.int32) for there, _ in neighbours))

    up_flow = (flow(0, spec, below1, up), flow(5, tile2, below2, up))
    tile_flow = (flow(1, spec, right1, left), flow(6, tile2, right2, left))
    diag_flow = (flow(2, below1, diag1, left), flow(7, below2, diag2, left))
    give_flow = (flow(3, give1, got1, right), flow(8, give2, got2, right))
    down_flow = (flow(4, down1, above1, down), flow(9, down2, above2, down))

    def meta_copy():
        return pltpu.make_async_remote_copy(
            src_ref=meta, dst_ref=left_dr, send_sem=meta_sem.at[0], recv_sem=meta_sem.at[1],
            device_id=right, device_id_type=MESH,
        )

    @pl.when(has_right)
    def _():
        meta_copy().start()

    def first_sends(k):
        @pl.when(has_up)
        def _():
            up_flow[0](k).start()

        @pl.when(has_left)
        def _():
            tile_flow[0](k).start()

    each(first_sends)

    @pl.when(jnp.logical_not(has_down))
    def _():
        for ref in (below1, below2, diag1, diag2):
            ref[...] = jnp.zeros_like(ref)

    @pl.when(jnp.logical_not(has_right))
    def _():
        for ref in (right1, right2, diag1, diag2):
            ref[...] = jnp.zeros_like(ref)

    @pl.when(jnp.logical_not(has_left))
    def _():
        for ref in (got1, got2, left_dr):
            ref[...] = jnp.zeros_like(ref)

    @pl.when(jnp.logical_not(has_up))
    def _():
        for ref in (above1, above2):
            ref[...] = jnp.zeros_like(ref)

    block = 128
    shape = (block, width)

    def wrapped(value):
        return jnp.where(value >= width, value - width, value)

    def one_hot(mask):
        return jnp.where(mask, 1.0, 0.0).astype(BF16)

    def columns_of(i):
        at = iota(shape, 0) + i * block
        hot[0, ds(i, block)] = one_hot(iota(shape, 1) == wrapped(at + dr))
        hot[1, ds(i, block)] = one_hot(iota(shape, 1) == wrapped(at + dc))

    each(columns_of, width // block)

    def rows_hot(i, shift):
        return one_hot(iota(shape, 0) + i * block == wrapped(iota(shape, 1) + shift))

    def tables(i):
        top, low = ds(i, block), ds(i, block, width)
        near, far = pl.ds(0, width), pl.ds(width, width)

        def put(ref, cos, sin, top_sign, low_sign):
            ref[top, near] = cos.astype(BF16)
            ref[low, far] = cos.astype(BF16)
            ref[top, far] = (top_sign * sin).astype(BF16)
            ref[low, near] = (low_sign * sin).astype(BF16)

        hot_rows = rows_hot(i, dc)
        put(fwd_right, dot(hot_rows, cosine[...]), dot(hot_rows, sine[...]), 1.0, -1.0)
        hot_rows = rows_hot(i, dr)
        put(back_left, dot(hot_rows, cosine[...]), dot(hot_rows, sine[...]), 1.0, -1.0)
        cos, sin = cosine[ds(i, block)], sine[ds(i, block)]
        put(fwd_left, dot(cos, hot[0]), dot(sin, hot[0]), -1.0, 1.0)
        put(back_right, dot(cos, hot[1]), dot(sin, hot[1]), -1.0, 1.0)

    each(tables, width // block)

    def three(value):
        high = value.astype(BF16)
        rest = value - high.astype(F32)
        middle = rest.astype(BF16)
        return high, middle, (rest - middle.astype(F32)).astype(BF16)

    for plane in range(2):
        def pupil_columns(i):
            parts = three(pupil[plane, ds(i, block)])
            moved = [dot(part, hot[1]) for part in parts]
            f1[ds(i, block)] = moved[0].astype(BF16)
            f1[ds(i, block, width)] = moved[1].astype(BF16)
            f2[ds(i, block)] = moved[2].astype(BF16)

        each(pupil_columns, width // block)

        def pupil_rows(i):
            hot_rows = rows_hot(i, dr)
            high = dot(hot_rows, f1[0:width])
            middle = dot(hot_rows, f1[width : 2 * width])
            pup[plane, ds(i, block)] = high + middle + dot(hot_rows, f2[0:width])

        each(pupil_rows, width // block)

    def masks(k):
        row = iota((size, width), 0) + k * size
        return row, row < dr, iota((size, width), 1) < dc

    def window(k, tile, below, right_tile, diag):
        _, low, far = masks(k)
        rows = ds(k)
        planes = [
            jnp.where(
                far,
                jnp.where(low, diag[p, rows], right_tile[p, rows]),
                jnp.where(low, below[p, rows], tile[p, rows]),
            )
            for p in range(2)
        ]
        pr, pi = pup[0, rows], pup[1, rows]
        field_real = planes[0] * pr - planes[1] * pi
        field_imag = planes[0] * pi + planes[1] * pr
        both = jnp.concatenate([field_real, field_imag], axis=1).astype(BF16)
        first = dot(both, fwd_right[...])
        f1[rows] = first[:, :width].astype(BF16)
        f1[ds(k, size, width)] = first[:, width:].astype(BF16)

    def middle(i):
        rows, low = ds(i, block), ds(i, block, width)
        wave_real = dot(fwd_left[rows], f1[...])
        wave_imag = dot(fwd_left[low], f1[...])
        magnitude = jnp.sqrt(wave_real * wave_real + wave_imag * wave_imag)
        keep = 1.0 - amps[rows] / jnp.maximum(magnitude, floor_value)
        both = jnp.concatenate([wave_real * keep, wave_imag * keep], axis=1).astype(BF16)
        first = dot(both, back_right[...])
        f2[rows] = first[:, :width].astype(BF16)
        f2[low] = first[:, width:].astype(BF16)

    tiles = (spec, tile2, out)
    for sweep in range(SWEEPS):
        tile, following = tiles[sweep], tiles[sweep + 1]
        below, right_tile, diag = ((below1, right1, diag1), (below2, right2, diag2))[sweep]
        give, got, lower, above = ((give1, got1, down1, above1), (give2, got2, down2, above2))[sweep]

        def relay(k):
            @pl.when(has_down)
            def _():
                up_flow[sweep](k).wait_recv()

                @pl.when(has_left)
                def _():
                    diag_flow[sweep](k).start()

        def consume(k):
            @pl.when(has_right)
            def _():
                tile_flow[sweep](k).wait_recv()

                @pl.when(has_down)
                def _():
                    diag_flow[sweep](k).wait_recv()

            window(k, tile, below, right_tile, diag)

        relay(0)

        def gather(k):
            relay(k + 1)
            consume(k)

        each(gather, CHUNKS - 1)
        consume(CHUNKS - 1)
        each(middle, width // block)

        def piece(k):
            _, _, far = masks(k)
            rows = ds(k)
            back_real = dot(back_left[rows], f2[...])
            back_imag = dot(back_left[ds(k, size, width)], f2[...])
            pr, pi = pup[0, rows], pup[1, rows]
            grads = (
                (back_real * pr + back_imag * pi) * live,
                (back_imag * pr - back_real * pi) * live,
            )
            for p in range(2):
                give[p, rows] = jnp.where(far, grads[p], 0.0)
                own[p, rows] = jnp.where(far, 0.0, grads[p])

            @pl.when(has_right)
            def _():
                give_flow[sweep](k).start()

        each(piece)

        if sweep == 0:
            @pl.when(has_left)
            def _():
                meta_copy().wait_recv()

        def pass_down(k):
            row, low, _ = masks(k)
            rows = ds(k)

            @pl.when(has_left)
            def _():
                give_flow[sweep](k).wait_recv()

            left_low = row.astype(F32) < left_dr[0:1, :]
            for p in range(2):
                mine, theirs = own[p, rows], got[p, rows]
                lower[p, rows] = jnp.where(low, mine, 0.0) + jnp.where(left_low, theirs, 0.0)
                kept = jnp.where(low, 0.0, mine) + jnp.where(left_low, 0.0, theirs)
                following[p, rows] = tile[p, rows] - step_size * kept

            @pl.when(has_down)
            def _():
                down_flow[sweep](k).start()

        each(pass_down)

        def finish(k):
            rows = ds(k)

            @pl.when(has_up)
            def _():
                down_flow[sweep](k).wait_recv()

            for p in range(2):
                following[p, rows] = following[p, rows] - step_size * above[p, rows]
            if sweep + 1 < SWEEPS:
                @pl.when(has_up)
                def _():
                    up_flow[sweep + 1](k).start()

                @pl.when(has_left)
                def _():
                    tile_flow[sweep + 1](k).start()

        each(finish)

    @pl.when(has_right)
    def _():
        meta_copy().wait_send()

    def sent(k):
        for sweep in range(SWEEPS):
            @pl.when(has_up)
            def _():
                up_flow[sweep](k).wait_send()

            @pl.when(has_left)
            def _():
                tile_flow[sweep](k).wait_send()

                @pl.when(has_down)
                def _():
                    diag_flow[sweep](k).wait_send()

            @pl.when(has_right)
            def _():
                give_flow[sweep](k).wait_send()

            @pl.when(has_down)
            def _():
                down_flow[sweep](k).wait_send()

    each(sent)


def on_device(n_row, n_col, spectrum, pupil, amplitudes, offsets, counts):
    width = pupil.shape[1]
    amps = amplitudes[0, 0, 0]
    place = offsets[0, 0, 0]
    live = (counts[0, 0] > 0).astype(jnp.int32)
    offs = jnp.concatenate([place, live[None]])
    meta = jnp.broadcast_to(place[0].astype(F32), (8, width))
    cosine, sine = dft_tables(width)
    plane = pltpu.VMEM((2, width, width), F32)
    table = pltpu.VMEM((2 * width, 2 * width), BF16)
    stage = pltpu.VMEM((2 * width, width), BF16)
    vmem = pl.BlockSpec(memory_space=pltpu.VMEM)
    return pl.pallas_call(
        functools.partial(kernel, n_row, n_col),
        out_shape=jax.ShapeDtypeStruct(spectrum.shape, F32),
        in_specs=[pl.BlockSpec(memory_space=pltpu.SMEM)] + [vmem] * 6,
        out_specs=vmem,
        scratch_shapes=[plane] * 17
        + [table] * 4
        + [stage] * 2
        + [
            pltpu.VMEM((2, width, width), BF16),
            pltpu.VMEM((8, width), F32),
            pltpu.SemaphoreType.DMA((5 * SWEEPS, CHUNKS)),
            pltpu.SemaphoreType.DMA((5 * SWEEPS, CHUNKS)),
            pltpu.SemaphoreType.DMA((2,)),
        ],
        compiler_params=pltpu.CompilerParams(
            collective_id=0, has_side_effects=True, vmem_limit_bytes=66 * 1000 * 1000
        ),
    )(offs, meta, spectrum, pupil, amps, cosine, sine)


def solution(mesh):
    in_specs = (
        P(None, "row", "col"),
        P(),
        P("row", "col", None, None, None),
        P("row", "col", None, None),
        P("row", "col"),
    )
    return jax.shard_map(
        functools.partial(on_device, mesh.shape["row"], mesh.shape["col"]),
        mesh=mesh, in_specs=in_specs, out_specs=P(None, "row", "col"), check_vma=False,
    )
```

```python
import functools
import math

import jax
import jax.numpy as jnp
import numpy as np
from jax import lax
from jax.experimental import pallas as pl
from jax.experimental.pallas import tpu as pltpu
from jax.sharding import PartitionSpec as P

SWEEPS = 2
CHUNKS = 16
LAG = 4

step_size = 0.5
floor_value = 0.05

MESH = pl.DeviceIdType.MESH
BF16 = jnp.bfloat16
F32 = jnp.float32


def dft_tables(width):
    index = np.arange(width)
    angle = (index[:, None] * index[None, :] % width) * (2.0 * math.pi / width)
    scale = 1.0 / math.sqrt(width)
    return (
        jnp.asarray((np.cos(angle) * scale).astype(np.float32).astype(BF16)),
        jnp.asarray((np.sin(angle) * scale).astype(np.float32).astype(BF16)),
    )


def dot(a, b):
    return jnp.dot(a, b, preferred_element_type=F32)


def iota(shape, axis):
    return lax.broadcasted_iota(jnp.int32, shape, axis)


def kernel(
    n_row, n_col, place, count, spec, pupil_in, amps_in, cosine_in, sine_in, out,
    below1, right1, diag1, give1, got1, own, down1, above1, tile2,
    below2, right2, diag2, give2, got2, down2, above2,
    pup, fwd_right, fwd_left, back_right, back_left, f1, f2, hot, left_dr, send, recv, meta_sem,
    meta, pupil, amps, cosine, sine, load,
):
    width = spec.shape[1]
    size = width // CHUNKS
    r, c = lax.axis_index("row"), lax.axis_index("col")
    has_up, has_down = r > 0, r < n_row - 1
    has_left, has_right = c > 0, c < n_col - 1
    up = (lax.rem(r + n_row - 1, n_row), c)
    down = (lax.rem(r + 1, n_row), c)
    left = (r, lax.rem(c + n_col - 1, n_col))
    right = (r, lax.rem(c + 1, n_col))
    dr, dc = place[0], place[1]
    live = jnp.where(count[0] > 0, 1.0, 0.0)
    loads = [
        pltpu.make_async_copy(source, target, load.at[at])
        for at, (source, target) in enumerate(
            ((cosine_in, cosine), (sine_in, sine), (pupil_in, pupil), (amps_in, amps))
        )
    ]
    for copy in loads:
        copy.start()
    meta[...] = jnp.zeros_like(meta) + dr.astype(F32)

    def ds(k, block=size, base=0):
        return pl.ds(pl.multiple_of(base + k * block, 8), block)

    def flow(kind, src, dst, device):
        def copy(k):
            return pltpu.make_async_remote_copy(
                src_ref=src.at[:, ds(k), :], dst_ref=dst.at[:, ds(k), :],
                send_sem=send.at[kind, k], recv_sem=recv.at[kind, k],
                device_id=device, device_id_type=MESH,
            )
        return copy

    def each(body, count=CHUNKS):
        def step(k, carry):
            body(k)
            return carry
        lax.fori_loop(0, count, step, 0)

    neighbours = ((has_up, up), (has_down, down), (has_left, left), (has_right, right))
    barrier = pltpu.get_barrier_semaphore()
    for there, device in neighbours:
        @pl.when(there)
        def _():
            pl.semaphore_signal(barrier, inc=1, device_id=device, device_id_type=MESH)
    pl.semaphore_wait(barrier, sum(there.astype(jnp.int32) for there, _ in neighbours))

    up_flow = (flow(0, spec, below1, up), flow(5, tile2, below2, up))
    tile_flow = (flow(1, spec, right1, left), flow(6, tile2, right2, left))
    diag_flow = (flow(2, below1, diag1, left), flow(7, below2, diag2, left))
    give_flow = (flow(3, give1, got1, right), flow(8, give2, got2, right))
    down_flow = (flow(4, down1, above1, down), flow(9, down2, above2, down))

    def meta_copy():
        return pltpu.make_async_remote_copy(
            src_ref=meta, dst_ref=left_dr, send_sem=meta_sem.at[0], recv_sem=meta_sem.at[1],
            device_id=right, device_id_type=MESH,
        )

    def first_sends(k):
        @pl.when(has_up)
        def _():
            up_flow[0](k).start()

        @pl.when(has_left)
        def _():
            tile_flow[0](k).start()

    each(first_sends)

    @pl.when(jnp.logical_not(has_down))
    def _():
        for ref in (below1, below2, diag1, diag2):
            ref[...] = jnp.zeros_like(ref)

    @pl.when(jnp.logical_not(has_right))
    def _():
        for ref in (right1, right2, diag1, diag2):
            ref[...] = jnp.zeros_like(ref)

    @pl.when(jnp.logical_not(has_left))
    def _():
        for ref in (got1, got2, left_dr):
            ref[...] = jnp.zeros_like(ref)

    @pl.when(jnp.logical_not(has_up))
    def _():
        for ref in (above1, above2):
            ref[...] = jnp.zeros_like(ref)

    @pl.when(has_right)
    def _():
        meta_copy().start()

    block = 128
    shape = (block, width)

    def wrapped(value):
        return jnp.where(value >= width, value - width, value)

    def one_hot(mask):
        return jnp.where(mask, 1.0, 0.0).astype(BF16)

    def columns_of(i):
        at = iota(shape, 0) + i * block
        hot[0, ds(i, block)] = one_hot(iota(shape, 1) == wrapped(at + dr))
        hot[1, ds(i, block)] = one_hot(iota(shape, 1) == wrapped(at + dc))

    each(columns_of, width // block)

    def rows_hot(i, shift):
        return one_hot(iota(shape, 0) + i * block == wrapped(iota(shape, 1) + shift))

    def tables(i):
        top, low = ds(i, block), ds(i, block, width)
        near, far = pl.ds(0, width), pl.ds(width, width)

        def put(ref, cos, sin, top_sign, low_sign):
            ref[top, near] = cos.astype(BF16)
            ref[low, far] = cos.astype(BF16)
            ref[top, far] = (top_sign * sin).astype(BF16)
            ref[low, near] = (low_sign * sin).astype(BF16)

        hot_rows = rows_hot(i, dc)
        put(fwd_right, dot(hot_rows, cosine[...]), dot(hot_rows, sine[...]), 1.0, -1.0)
        hot_rows = rows_hot(i, dr)
        put(back_left, dot(hot_rows, cosine[...]), dot(hot_rows, sine[...]), 1.0, -1.0)
        cos, sin = cosine[ds(i, block)], sine[ds(i, block)]
        put(fwd_left, dot(cos, hot[0]), dot(sin, hot[0]), -1.0, 1.0)
        put(back_right, dot(cos, hot[1]), dot(sin, hot[1]), -1.0, 1.0)

    for copy in loads:
        copy.wait()
    each(tables, width // block)

    def three(value):
        high = value.astype(BF16)
        rest = value - high.astype(F32)
        middle = rest.astype(BF16)
        return high, middle, (rest - middle.astype(F32)).astype(BF16)

    for plane in range(2):
        def pupil_columns(i):
            parts = three(pupil[plane, ds(i, block)])
            moved = [dot(part, hot[1]) for part in parts]
            f1[ds(i, block)] = moved[0].astype(BF16)
            f1[ds(i, block, width)] = moved[1].astype(BF16)
            f2[ds(i, block)] = moved[2].astype(BF16)

        each(pupil_columns, width // block)

        def pupil_rows(i):
            hot_rows = rows_hot(i, dr)
            high = dot(hot_rows, f1[0:width])
            middle = dot(hot_rows, f1[width : 2 * width])
            pup[plane, ds(i, block)] = high + middle + dot(hot_rows, f2[0:width])

        each(pupil_rows, width // block)

    def masks(k):
        row = iota((size, width), 0) + k * size
        return row, row < dr, iota((size, width), 1) < dc

    def window(k, tile, below, right_tile, diag):
        _, low, far = masks(k)
        rows = ds(k)
        planes = [
            jnp.where(
                far,
                jnp.where(low, diag[p, rows], right_tile[p, rows]),
                jnp.where(low, below[p, rows], tile[p, rows]),
            )
            for p in range(2)
        ]
        pr, pi = pup[0, rows], pup[1, rows]
        field_real = planes[0] * pr - planes[1] * pi
        field_imag = planes[0] * pi + planes[1] * pr
        both = jnp.concatenate([field_real, field_imag], axis=1).astype(BF16)
        first = dot(both, fwd_right[...])
        f1[rows] = first[:, :width].astype(BF16)
        f1[ds(k, size, width)] = first[:, width:].astype(BF16)

    wide = width // 2

    def middle(i):
        rows, low = ds(i, wide), ds(i, wide, width)
        wave = dot(jnp.concatenate([fwd_left[rows], fwd_left[low]], axis=0), f1[...])
        wave_real, wave_imag = wave[:wide], wave[wide:]
        magnitude = jnp.sqrt(wave_real * wave_real + wave_imag * wave_imag)
        keep = 1.0 - amps[rows] / jnp.maximum(magnitude, floor_value)
        both = jnp.concatenate([wave_real * keep, wave_imag * keep], axis=1).astype(BF16)
        first = dot(both, back_right[...])
        f2[rows] = first[:, :width].astype(BF16)
        f2[low] = first[:, width:].astype(BF16)

    tiles = (spec, tile2, out)
    for sweep in range(SWEEPS):
        tile, following = tiles[sweep], tiles[sweep + 1]
        below, right_tile, diag = ((below1, right1, diag1), (below2, right2, diag2))[sweep]
        give, got, lower, above = ((give1, got1, down1, above1), (give2, got2, down2, above2))[sweep]

        def relay(k):
            @pl.when(has_down)
            def _():
                up_flow[sweep](k).wait_recv()

                @pl.when(has_left)
                def _():
                    diag_flow[sweep](k).start()

        def consume(k):
            @pl.when(has_right)
            def _():
                tile_flow[sweep](k).wait_recv()

                @pl.when(has_down)
                def _():
                    diag_flow[sweep](k).wait_recv()

            window(k, tile, below, right_tile, diag)

        relay(0)

        def gather(k):
            relay(k + 1)
            consume(k)

        each(gather, CHUNKS - 1)
        consume(CHUNKS - 1)
        each(middle, width // wide)

        def piece(k):
            _, _, far = masks(k)
            rows = ds(k)
            low = ds(k, size, width)
            back = dot(jnp.concatenate([back_left[rows], back_left[low]], axis=0), f2[...])
            back_real, back_imag = back[:size], back[size:]
            pr, pi = pup[0, rows], pup[1, rows]
            grads = (
                (back_real * pr + back_imag * pi) * live,
                (back_imag * pr - back_real * pi) * live,
            )
            for p in range(2):
                give[p, rows] = jnp.where(far, grads[p], 0.0)
                own[p, rows] = jnp.where(far, 0.0, grads[p])

            @pl.when(has_right)
            def _():
                give_flow[sweep](k).start()

        each(piece, LAG)

        if sweep == 0:
            @pl.when(has_left)
            def _():
                meta_copy().wait_recv()

        def pass_down(k):
            row, low, _ = masks(k)
            rows = ds(k)

            @pl.when(has_left)
            def _():
                give_flow[sweep](k).wait_recv()

            left_low = row.astype(F32) < left_dr[0:1, :]
            for p in range(2):
                mine, theirs = own[p, rows], got[p, rows]
                lower[p, rows] = jnp.where(low, mine, 0.0) + jnp.where(left_low, theirs, 0.0)
                kept = jnp.where(low, 0.0, mine) + jnp.where(left_low, 0.0, theirs)
                following[p, rows] = tile[p, rows] - step_size * kept

            @pl.when(has_down)
            def _():
                down_flow[sweep](k).start()

        def both_ways(k):
            piece(k + LAG)
            pass_down(k)

        def last_down(k):
            pass_down(k + CHUNKS - LAG)

        each(both_ways, CHUNKS - LAG)
        each(last_down, LAG)

        def finish(k):
            rows = ds(k)

            @pl.when(has_up)
            def _():
                down_flow[sweep](k).wait_recv()

            for p in range(2):
                following[p, rows] = following[p, rows] - step_size * above[p, rows]
            if sweep + 1 < SWEEPS:
                @pl.when(has_up)
                def _():
                    up_flow[sweep + 1](k).start()

                @pl.when(has_left)
                def _():
                    tile_flow[sweep + 1](k).start()

        each(finish)

    @pl.when(has_right)
    def _():
        meta_copy().wait_send()

    def sent(k):
        for sweep in range(SWEEPS):
            @pl.when(has_up)
            def _():
                up_flow[sweep](k).wait_send()

            @pl.when(has_left)
            def _():
                tile_flow[sweep](k).wait_send()

                @pl.when(has_down)
                def _():
                    diag_flow[sweep](k).wait_send()

            @pl.when(has_right)
            def _():
                give_flow[sweep](k).wait_send()

            @pl.when(has_down)
            def _():
                down_flow[sweep](k).wait_send()

    each(sent)


def on_device(n_row, n_col, spectrum, pupil, amplitudes, offsets, counts):
    width = pupil.shape[1]
    amps = amplitudes[0, 0, 0]
    place = offsets.reshape(-1)
    count = counts.reshape(-1)
    cosine, sine = dft_tables(width)
    plane = pltpu.VMEM((2, width, width), F32)
    table = pltpu.VMEM((2 * width, 2 * width), BF16)
    stage = pltpu.VMEM((2 * width, width), BF16)
    vmem = pl.BlockSpec(memory_space=pltpu.VMEM)
    return pl.pallas_call(
        functools.partial(kernel, n_row, n_col),
        out_shape=jax.ShapeDtypeStruct(spectrum.shape, F32),
        in_specs=[pl.BlockSpec(memory_space=pltpu.SMEM)] * 2
        + [vmem]
        + [pl.BlockSpec(memory_space=pltpu.MemorySpace.HBM)] * 4,
        out_specs=vmem,
        scratch_shapes=[plane] * 17
        + [table] * 4
        + [stage] * 2
        + [
            pltpu.VMEM((2, width, width), BF16),
            pltpu.VMEM((8, width), F32),
            pltpu.SemaphoreType.DMA((5 * SWEEPS, CHUNKS)),
            pltpu.SemaphoreType.DMA((5 * SWEEPS, CHUNKS)),
            pltpu.SemaphoreType.DMA((2,)),
            pltpu.VMEM((8, width), F32),
            plane,
            pltpu.VMEM((width, width), F32),
            pltpu.VMEM((width, width), BF16),
            pltpu.VMEM((width, width), BF16),
            pltpu.SemaphoreType.DMA((4,)),
        ],
        compiler_params=pltpu.CompilerParams(
            collective_id=0, has_side_effects=True, vmem_limit_bytes=66 * 1000 * 1000
        ),
    )(place, count, spectrum, pupil, amps, cosine, sine)


def solution(mesh):
    in_specs = (
        P(None, "row", "col"),
        P(),
        P("row", "col", None, None, None),
        P("row", "col", None, None),
        P("row", "col"),
    )
    return jax.shard_map(
        functools.partial(on_device, mesh.shape["row"], mesh.shape["col"]),
        mesh=mesh, in_specs=in_specs, out_specs=P(None, "row", "col"), check_vma=False,
    )
```

```python
import functools
import math

import jax
import jax.numpy as jnp
import numpy as np
from jax import lax
from jax.experimental import pallas as pl
from jax.experimental.pallas import tpu as pltpu
from jax.sharding import PartitionSpec as P

SWEEPS = 2
CHUNKS = 16
LAG = 4

step_size = 0.5
floor_value = 0.05

MESH = pl.DeviceIdType.MESH
BF16 = jnp.bfloat16
F32 = jnp.float32


def dft_tables(width):
    index = np.arange(width)
    angle = (index[:, None] * index[None, :] % width) * (2.0 * math.pi / width)
    scale = 1.0 / math.sqrt(width)
    return (
        jnp.asarray((np.cos(angle) * scale).astype(np.float32).astype(BF16)),
        jnp.asarray((np.sin(angle) * scale).astype(np.float32).astype(BF16)),
    )


def dot(a, b):
    return jnp.dot(a, b, preferred_element_type=F32)


def iota(shape, axis):
    return lax.broadcasted_iota(jnp.int32, shape, axis)


def kernel(
    n_row, n_col, place, count, spec, pupil_in, amps_in, cosine_in, sine_in, out,
    below1, right1, mix1, give1, got1, own, down1, above1, tile2,
    below2, right2, mix2, give2, got2, down2, above2,
    pup, fwd_right, fwd_left, back_right, back_left, f1, f2, hot, left_dr, send, recv, meta_sem,
    meta, pupil, amps, cosine, sine, load,
):
    width = spec.shape[1]
    size = width // CHUNKS
    r, c = lax.axis_index("row"), lax.axis_index("col")
    has_up, has_down = r > 0, r < n_row - 1
    has_left, has_right = c > 0, c < n_col - 1
    up = (lax.rem(r + n_row - 1, n_row), c)
    down = (lax.rem(r + 1, n_row), c)
    left = (r, lax.rem(c + n_col - 1, n_col))
    right = (r, lax.rem(c + 1, n_col))
    dr, dc = place[0], place[1]
    live = jnp.where(count[0] > 0, 1.0, 0.0)
    loads = [
        pltpu.make_async_copy(source, target, load.at[at])
        for at, (source, target) in enumerate(
            ((cosine_in, cosine), (sine_in, sine), (pupil_in, pupil), (amps_in, amps))
        )
    ]
    for copy in loads:
        copy.start()
    meta[...] = jnp.zeros_like(meta) + dr.astype(F32)

    def ds(k, block=size, base=0):
        return pl.ds(pl.multiple_of(base + k * block, 8), block)

    def flow(kind, src, dst, device):
        def copy(k):
            return pltpu.make_async_remote_copy(
                src_ref=src.at[:, ds(k), :], dst_ref=dst.at[:, ds(k), :],
                send_sem=send.at[kind, k], recv_sem=recv.at[kind, k],
                device_id=device, device_id_type=MESH,
            )
        return copy

    def each(body, count=CHUNKS):
        def step(k, carry):
            body(k)
            return carry
        lax.fori_loop(0, count, step, 0)

    neighbours = ((has_up, up), (has_down, down), (has_left, left), (has_right, right))
    barrier = pltpu.get_barrier_semaphore()
    for there, device in neighbours:
        @pl.when(there)
        def _():
            pl.semaphore_signal(barrier, inc=1, device_id=device, device_id_type=MESH)
    pl.semaphore_wait(barrier, sum(there.astype(jnp.int32) for there, _ in neighbours))

    up_flow = (flow(0, spec, below1, up), flow(3, tile2, below2, up))
    left_flow = (flow(1, mix1, right1, left), flow(2, mix2, right2, left))
    give_flow = (flow(4, give1, got1, right), flow(5, give2, got2, right))
    down_flow = (flow(6, down1, above1, down), flow(7, down2, above2, down))

    def meta_copy():
        return pltpu.make_async_remote_copy(
            src_ref=meta, dst_ref=left_dr, send_sem=meta_sem.at[0], recv_sem=meta_sem.at[1],
            device_id=right, device_id_type=MESH,
        )

    def first_sends(k):
        @pl.when(has_up)
        def _():
            up_flow[0](k).start()

    each(first_sends)

    @pl.when(jnp.logical_not(has_down))
    def _():
        for ref in (below1, below2):
            ref[...] = jnp.zeros_like(ref)

    @pl.when(jnp.logical_not(has_right))
    def _():
        for ref in (right1, right2):
            ref[...] = jnp.zeros_like(ref)

    @pl.when(jnp.logical_not(has_left))
    def _():
        for ref in (got1, got2, left_dr):
            ref[...] = jnp.zeros_like(ref)

    @pl.when(jnp.logical_not(has_up))
    def _():
        for ref in (above1, above2):
            ref[...] = jnp.zeros_like(ref)

    @pl.when(has_right)
    def _():
        meta_copy().start()

    block = 128
    shape = (block, width)

    def wrapped(value):
        return jnp.where(value >= width, value - width, value)

    def one_hot(mask):
        return jnp.where(mask, 1.0, 0.0).astype(BF16)

    def columns_of(i):
        at = iota(shape, 0) + i * block
        hot[0, ds(i, block)] = one_hot(iota(shape, 1) == wrapped(at + dr))
        hot[1, ds(i, block)] = one_hot(iota(shape, 1) == wrapped(at + dc))

    each(columns_of, width // block)

    def rows_hot(i, shift):
        return one_hot(iota(shape, 0) + i * block == wrapped(iota(shape, 1) + shift))

    def tables(i):
        top, low = ds(i, block), ds(i, block, width)
        near, far = pl.ds(0, width), pl.ds(width, width)

        def put(ref, cos, sin, top_sign, low_sign):
            ref[top, near] = cos.astype(BF16)
            ref[low, far] = cos.astype(BF16)
            ref[top, far] = (top_sign * sin).astype(BF16)
            ref[low, near] = (low_sign * sin).astype(BF16)

        hot_rows = rows_hot(i, dc)
        put(fwd_right, dot(hot_rows, cosine[...]), dot(hot_rows, sine[...]), 1.0, -1.0)
        hot_rows = rows_hot(i, dr)
        put(back_left, dot(hot_rows, cosine[...]), dot(hot_rows, sine[...]), 1.0, -1.0)
        cos, sin = cosine[ds(i, block)], sine[ds(i, block)]
        put(fwd_left, dot(cos, hot[0]), dot(sin, hot[0]), -1.0, 1.0)
        put(back_right, dot(cos, hot[1]), dot(sin, hot[1]), -1.0, 1.0)

    for copy in loads:
        copy.wait()
    each(tables, width // block)

    def three(value):
        high = value.astype(BF16)
        rest = value - high.astype(F32)
        middle = rest.astype(BF16)
        return high, middle, (rest - middle.astype(F32)).astype(BF16)

    for plane in range(2):
        def pupil_columns(i):
            parts = three(pupil[plane, ds(i, block)])
            moved = [dot(part, hot[1]) for part in parts]
            f1[ds(i, block)] = moved[0].astype(BF16)
            f1[ds(i, block, width)] = moved[1].astype(BF16)
            f2[ds(i, block)] = moved[2].astype(BF16)

        each(pupil_columns, width // block)

        def pupil_rows(i):
            hot_rows = rows_hot(i, dr)
            high = dot(hot_rows, f1[0:width])
            middle = dot(hot_rows, f1[width : 2 * width])
            pup[plane, ds(i, block)] = high + middle + dot(hot_rows, f2[0:width])

        each(pupil_rows, width // block)

    def masks(k):
        row = iota((size, width), 0) + k * size
        return row, row < dr, iota((size, width), 1) < dc

    def window(k, tile, below, right_tile):
        _, low, far = masks(k)
        rows = ds(k)
        planes = [
            jnp.where(
                far, right_tile[p, rows], jnp.where(low, below[p, rows], tile[p, rows])
            )
            for p in range(2)
        ]
        pr, pi = pup[0, rows], pup[1, rows]
        field_real = planes[0] * pr - planes[1] * pi
        field_imag = planes[0] * pi + planes[1] * pr
        both = jnp.concatenate([field_real, field_imag], axis=1).astype(BF16)
        first = dot(both, fwd_right[...])
        f1[rows] = first[:, :width].astype(BF16)
        f1[ds(k, size, width)] = first[:, width:].astype(BF16)

    wide = width // 2

    def middle(i):
        rows, low = ds(i, wide), ds(i, wide, width)
        wave = dot(jnp.concatenate([fwd_left[rows], fwd_left[low]], axis=0), f1[...])
        wave_real, wave_imag = wave[:wide], wave[wide:]
        magnitude = jnp.sqrt(wave_real * wave_real + wave_imag * wave_imag)
        keep = 1.0 - amps[rows] / jnp.maximum(magnitude, floor_value)
        both = jnp.concatenate([wave_real * keep, wave_imag * keep], axis=1).astype(BF16)
        first = dot(both, back_right[...])
        f2[rows] = first[:, :width].astype(BF16)
        f2[low] = first[:, width:].astype(BF16)

    tiles = (spec, tile2, out)
    for sweep in range(SWEEPS):
        tile, following = tiles[sweep], tiles[sweep + 1]
        below, right_tile, mix = ((below1, right1, mix1), (below2, right2, mix2))[sweep]
        give, got, lower, above = ((give1, got1, down1, above1), (give2, got2, down2, above2))[sweep]

        def relay(k):
            @pl.when(has_down)
            def _():
                up_flow[sweep](k).wait_recv()

            @pl.when(has_left)
            def _():
                rows = ds(k)
                row, _, _ = masks(k)
                left_low = row.astype(F32) < left_dr[0:1, :]
                for p in range(2):
                    mix[p, rows] = jnp.where(left_low, below[p, rows], tile[p, rows])
                left_flow[sweep](k).start()

        def consume(k):
            @pl.when(has_right)
            def _():
                left_flow[sweep](k).wait_recv()

            window(k, tile, below, right_tile)

        if sweep == 0:
            @pl.when(has_left)
            def _():
                meta_copy().wait_recv()

        relay(0)

        def gather(k):
            relay(k + 1)
            consume(k)

        each(gather, CHUNKS - 1)
        consume(CHUNKS - 1)
        each(middle, width // wide)

        def piece(k):
            _, _, far = masks(k)
            rows = ds(k)
            low = ds(k, size, width)
            back = dot(jnp.concatenate([back_left[rows], back_left[low]], axis=0), f2[...])
            back_real, back_imag = back[:size], back[size:]
            pr, pi = pup[0, rows], pup[1, rows]
            grads = (
                (back_real * pr + back_imag * pi) * live,
                (back_imag * pr - back_real * pi) * live,
            )
            for p in range(2):
                give[p, rows] = jnp.where(far, grads[p], 0.0)
                own[p, rows] = jnp.where(far, 0.0, grads[p])

            @pl.when(has_right)
            def _():
                give_flow[sweep](k).start()

        each(piece, LAG)

        def pass_down(k):
            row, low, _ = masks(k)
            rows = ds(k)

            @pl.when(has_left)
            def _():
                give_flow[sweep](k).wait_recv()

            left_low = row.astype(F32) < left_dr[0:1, :]
            for p in range(2):
                mine, theirs = own[p, rows], got[p, rows]
                lower[p, rows] = jnp.where(low, mine, 0.0) + jnp.where(left_low, theirs, 0.0)
                kept = jnp.where(low, 0.0, mine) + jnp.where(left_low, 0.0, theirs)
                following[p, rows] = tile[p, rows] - step_size * kept

            @pl.when(has_down)
            def _():
                down_flow[sweep](k).start()

        def both_ways(k):
            piece(k + LAG)
            pass_down(k)

        def last_down(k):
            pass_down(k + CHUNKS - LAG)

        each(both_ways, CHUNKS - LAG)
        each(last_down, LAG)

        def finish(k):
            rows = ds(k)

            @pl.when(has_up)
            def _():
                down_flow[sweep](k).wait_recv()

            for p in range(2):
                following[p, rows] = following[p, rows] - step_size * above[p, rows]
            if sweep + 1 < SWEEPS:
                @pl.when(has_up)
                def _():
                    up_flow[sweep + 1](k).start()

        each(finish)

    @pl.when(has_right)
    def _():
        meta_copy().wait_send()

    def sent(k):
        for sweep in range(SWEEPS):
            @pl.when(has_up)
            def _():
                up_flow[sweep](k).wait_send()

            @pl.when(has_left)
            def _():
                left_flow[sweep](k).wait_send()

            @pl.when(has_right)
            def _():
                give_flow[sweep](k).wait_send()

            @pl.when(has_down)
            def _():
                down_flow[sweep](k).wait_send()

    each(sent)


def on_device(n_row, n_col, spectrum, pupil, amplitudes, offsets, counts):
    width = pupil.shape[1]
    amps = amplitudes[0, 0, 0]
    place = offsets.reshape(-1)
    count = counts.reshape(-1)
    cosine, sine = dft_tables(width)
    plane = pltpu.VMEM((2, width, width), F32)
    table = pltpu.VMEM((2 * width, 2 * width), BF16)
    stage = pltpu.VMEM((2 * width, width), BF16)
    vmem = pl.BlockSpec(memory_space=pltpu.VMEM)
    return pl.pallas_call(
        functools.partial(kernel, n_row, n_col),
        out_shape=jax.ShapeDtypeStruct(spectrum.shape, F32),
        in_specs=[pl.BlockSpec(memory_space=pltpu.SMEM)] * 2
        + [vmem]
        + [pl.BlockSpec(memory_space=pltpu.MemorySpace.HBM)] * 4,
        out_specs=vmem,
        scratch_shapes=[plane] * 17
        + [table] * 4
        + [stage] * 2
        + [
            pltpu.VMEM((2, width, width), BF16),
            pltpu.VMEM((8, width), F32),
            pltpu.SemaphoreType.DMA((4 * SWEEPS, CHUNKS)),
            pltpu.SemaphoreType.DMA((4 * SWEEPS, CHUNKS)),
            pltpu.SemaphoreType.DMA((2,)),
            pltpu.VMEM((8, width), F32),
            plane,
            pltpu.VMEM((width, width), F32),
            pltpu.VMEM((width, width), BF16),
            pltpu.VMEM((width, width), BF16),
            pltpu.SemaphoreType.DMA((4,)),
        ],
        compiler_params=pltpu.CompilerParams(
            collective_id=0, has_side_effects=True, vmem_limit_bytes=66 * 1000 * 1000
        ),
    )(place, count, spectrum, pupil, amps, cosine, sine)


def solution(mesh):
    in_specs = (
        P(None, "row", "col"),
        P(),
        P("row", "col", None, None, None),
        P("row", "col", None, None),
        P("row", "col"),
    )
    return jax.shard_map(
        functools.partial(on_device, mesh.shape["row"], mesh.shape["col"]),
        mesh=mesh, in_specs=in_specs, out_specs=P(None, "row", "col"), check_vma=False,
    )
```
